256 devices in a mesh: dp: 4 (over x), expert: 64 (over y, z, core).
Axes of the slice: x: 4, y: 4, z: 8, core: 2. Of those that a mesh axis runs over, the one named last changes fastest.
Arguments:
- tokens: bfloat16 [32768, 2048], P(('dp', 'expert')), may hold values from -24 to 24
- grad_out: bfloat16 [32768, 2048], P(('dp', 'expert')), may hold values from -0.125 to 0.125
- router_weight: bfloat16 [2048, 64], replicated, may hold values from -0.125 to 0.125
- expert_index: int32 [32768, 8], P(('dp', 'expert')), may hold values from 0 to 63, all different within a row; in each aligned block of 128 rows (0 to 127, 128 to 255, ...) at most 24 rows name the same one
- w_gate: bfloat16 [64, 2048, 768], P('expert'), may hold values from -0.125 to 0.125
- w_up: bfloat16 [64, 2048, 768], P('expert'), may hold values from -0.125 to 0.125
- w_down: bfloat16 [64, 768, 2048], P('expert'), may hold values from -0.21875 to 0.21875
Outputs:
- gate_grad: float32 [32768, 8], P(('dp', 'expert'))
- router_grad: float32 [2048, 64], P('expert')
The draws below stay inside these ranges and needn't reach their ends.
Inputs may be any that keep to these rules, and one draw needn't show every extreme that they name: `expert_index`: each row names 8 different experts. In each aligned block of 128 rows (the rows of one device) no expert is named by more than 24 rows, a bound that some blocks reach.
All inputs are finite; a program needn't handle non-finite values.
Results may differ from the reference program's by a relative error of at most 0.009.
Values may be sent and summed in bfloat16 or wider, within the bound.
No kernel may reach another device: no remote copies, remote signals or barrier semaphores. Data moves between devices by JAX's collectives and lax.ppermute only.
A program may use at most 128 MiB of HBM per device.

```python
import math
import jax
import jax.numpy as jnp
import numpy as np
from jax import lax

D = 2048
FF = 768
TOP = 8
TOK_DEV = 128
EXPERTS = 64
CAP = 24
TOKENS = 32768


def spiked(array, stream_key, source, target, shards_of, factor):
    def block_of(position):
        return (jnp.arange(array.shape[position]) // (array.shape[position] // shards_of)).reshape((-1,) + (1,) * (array.ndim - 1 - position))

    one_side = jax.random.permutation(stream_key, shards_of)[block_of(target)]
    second = (block_of(target) + shards_of // 2) % shards_of
    return jnp.where((block_of(source) == one_side) | (block_of(source) == second), factor * array, array)


def steps_of(stream_key, dims, shards, least, high):
    loudness = 1.0
    for dim, parts in shards:
        heights = jax.random.uniform(jax.random.fold_in(jax.random.fold_in(stream_key, 6), dim), (parts,), jnp.float32, least / len(shards), high / len(shards))
        loudness = loudness * jnp.repeat(jnp.exp(heights), dims[dim] // parts).reshape((-1,) + (1,) * (len(dims) - 1 - dim))
    return loudness


def deal_out(rng, own, number, rows, count, top, most, slope):
    ranking = jax.random.permutation(rng, count)
    heavy_load, common = portions_of(count, rows * top, most, slope, True), portions_of(count, rows * top, most, slope, False)
    places = jnp.arange(count)

    def named(sizes, rotation):
        used = int((sizes > 0).sum())
        fixed = max(1, used // 4)
        shifted = fixed + (places - fixed + rotation * (used - fixed)) % max(1, count - fixed)
        return jnp.zeros((count,), jnp.int32).at[ranking[jnp.where(places < fixed, places, shifted)]].set(jnp.asarray(sizes, jnp.int32))

    sizes = jnp.where(number % 4 == 0, named(heavy_load, number // 4), named(common, number - number // 4 - 1))
    mixed = jax.random.permutation(jax.random.fold_in(own, 3), count)
    donor, taker = mixed[0:count // 2 * 2:2], mixed[1:count // 2 * 2:2]
    margin = jnp.minimum(sizes[donor] - 1, most - sizes[taker]) // 2
    margin = jnp.where((donor == ranking[0]) | (taker == ranking[0]) | (sizes[taker] == 0), 0, jnp.maximum(margin, 0))
    shifted = jax.random.randint(jax.random.fold_in(own, 4), (count // 2,), 0, 1 << 20) % (margin + 1)
    sizes = sizes.at[donor].add(-shifted).at[taker].add(shifted)
    items = jnp.searchsorted(jnp.cumsum(sizes), jnp.arange(rows * top), side="right").astype(jnp.int32)
    listing = items.reshape(top, rows).T
    listing = listing[jax.random.permutation(jax.random.fold_in(own, 1), rows)]
    rotation = jax.random.randint(jax.random.fold_in(own, 2), (rows, 1), 0, top)
    return jnp.take_along_axis(listing, (jnp.arange(top)[None, :] + rotation) % top, axis=1)


def portions_of(number_of, total, bound, slope, full):
    weights = [(1 << 20) // math.isqrt(standing ** slope) + 1 for standing in range(1, number_of + 1)]
    largest = bound if full else min(bound, max(-(-total // number_of), total * weights[0] // sum(weights)))
    least = 1 if total - largest >= number_of - 1 else 0
    counts, rest = [largest] + [least] * (number_of - 1), total - largest - least * (number_of - 1)
    while rest > 0:
        movable = [i for i in range(1, number_of) if counts[i] < largest] or [i for i in range(1, number_of) if counts[i] < bound]
        whole, remaining = sum([weights[i] for i in movable]), rest
        for i in movable:
            extra = min(bound - counts[i], max(1, remaining * weights[i] // whole), rest)
            counts[i] = counts[i] + extra
            rest = rest - extra
    return np.array(counts)


def bell_draw(stream_key, dims, width, most, pieces=(), held_as=jnp.bfloat16):
    gain = steps_of(stream_key, dims, pieces, -0.22, 0.18) if pieces else 1.0
    result = jax.random.normal(stream_key, dims, jnp.float32) * width * gain
    return jnp.minimum(jnp.maximum(result, -most), most).astype(held_as)


def gaussian_with(key, extent, spread, bound, shards, heavy, held_as=jnp.bfloat16):
    values = spread * jax.random.normal(key, extent, jnp.float32)
    if shards:
        values = values * steps_of(key, extent, shards, -0.22, 0.18)
    return jnp.clip(spiked(values, jax.random.fold_in(key, 3), *heavy), -bound, bound).astype(held_as)


def setup_inputs(seed: int = 0) -> dict:
    keys = jax.random.split(jax.random.key(seed), 8)
    tokens = gaussian_with(keys[0], (TOKENS, D), 1.0, 24.0, ((0, 256),), (0, 1, 256, 6.0))
    grad_out = bell_draw(keys[1], (TOKENS, D), D ** -0.5, 0.125, ((0, 256),))
    router_weight = bell_draw(keys[2], (D, EXPERTS), D ** -0.5, 0.125)
    expert_index_keys = jax.random.split(jax.random.fold_in(keys[3], 1), TOKENS // TOK_DEV)
    expert_index_turns = jax.random.permutation(jax.random.fold_in(keys[3], 3), TOKENS // TOK_DEV)
    expert_index = jax.vmap(lambda own, number: deal_out(jax.random.fold_in(keys[3], 2), own, number, TOK_DEV, EXPERTS, TOP, CAP, 2))(expert_index_keys, expert_index_turns).reshape((TOKENS, TOP))
    w_gate = bell_draw(keys[4], (EXPERTS, D, FF), D ** -0.5, 0.125, ((0, 64),))
    w_up = bell_draw(keys[5], (EXPERTS, D, FF), D ** -0.5, 0.125, ((0, 64),))
    w_down = bell_draw(keys[6], (EXPERTS, FF, D), FF ** -0.5, 0.21875, ((0, 64),))
    return dict(tokens=tokens, grad_out=grad_out, router_weight=router_weight, expert_index=expert_index, w_gate=w_gate, w_up=w_up, w_down=w_down)


def slot_table(expert_index):
    blocks = expert_index.reshape(-1, TOK_DEV, TOP)
    labels = jnp.arange(EXPERTS, dtype=jnp.int32)
    hits = (blocks[..., None] == labels).astype(jnp.int32)
    per_token = jnp.sum(hits, axis=2)
    before = jnp.cumsum(per_token, axis=1) - per_token
    slot = jnp.sum(hits * before[:, :, None, :], axis=3)
    return slot.reshape(-1, TOP).astype(jnp.int32)


def reference(tokens, grad_out, router_weight, expert_index, w_gate, w_up, w_down):
    slot = slot_table(expert_index)
    blocks = TOKENS // TOK_DEV
    token_ids = jnp.broadcast_to(jnp.arange(TOKENS, dtype=jnp.int32)[:, None], (TOKENS, TOP))
    source = (token_ids // TOK_DEV).astype(jnp.int32)
    column = (source * CAP + slot).astype(jnp.int32)
    table = jnp.zeros((EXPERTS, blocks * CAP), jnp.int32).at[expert_index, column].set(token_ids)

    def one_expert(which):
        picked = table[which]
        rows = tokens[picked]
        gate_in = jnp.dot(rows, w_gate[which], preferred_element_type=jnp.float32)
        up_in = jnp.dot(rows, w_up[which], preferred_element_type=jnp.float32)
        hidden = (jax.nn.silu(gate_in) * up_in).astype(jnp.bfloat16)
        expert_out = jnp.dot(hidden, w_down[which], preferred_element_type=jnp.float32).astype(jnp.bfloat16)
        return jnp.sum(expert_out.astype(jnp.float32) * grad_out[picked].astype(jnp.float32), axis=1)

    dots = lax.map(one_expert, jnp.arange(EXPERTS, dtype=jnp.int32))
    gate_grad = dots[expert_index, column]

    logits = jnp.dot(tokens, router_weight, preferred_element_type=jnp.float32)
    chosen = jnp.take_along_axis(logits, expert_index, axis=1)
    weights = jnp.exp(chosen)
    gates = weights / jnp.sum(weights, axis=1, keepdims=True)
    mean_term = jnp.sum(gates * gate_grad, axis=1, keepdims=True)
    logit_grad = gates * (gate_grad - mean_term)
    labels = jnp.arange(EXPERTS, dtype=jnp.int32)
    hits = (expert_index[:, :, None] == labels).astype(jnp.float32)
    dense = jnp.sum(logit_grad[:, :, None] * hits, axis=1)
    router_grad = jnp.dot(tokens.astype(jnp.float32).T, dense, precision=lax.Precision.HIGHEST)
    return gate_grad, router_grad
```

```python
import functools

import jax
import jax.numpy as jnp
from jax import lax
from jax.experimental import pallas as pl
from jax.experimental.pallas import tpu as pltpu
from jax.sharding import Mesh, PartitionSpec as P


NY, NZ, NC = 4, 8, 2
CAP = 24
VMEM = 48 * 1024 * 1024


def place_kernel(tok_ref, idx_ref, out_ref):
    rows, width = tok_ref.shape
    out_ref[:, :width] = tok_ref[...]
    lane = lax.broadcasted_iota(jnp.int32, (rows, 128), 1)
    hit = jnp.zeros((rows, 128), jnp.float32)
    for k in range(idx_ref.shape[1]):
        hit = hit + (idx_ref[:, k : k + 1] == lane).astype(jnp.float32)
    earlier = lax.broadcasted_iota(jnp.int32, (rows, rows), 0) > lax.broadcasted_iota(
        jnp.int32, (rows, rows), 1
    )
    before = jnp.dot(
        earlier.astype(jnp.bfloat16),
        hit.astype(jnp.bfloat16),
        preferred_element_type=jnp.float32,
    )
    out_ref[:, width:] = jnp.where(hit > 0.0, before, -1.0).astype(jnp.bfloat16)


def relative(r):
    return r // NC, r % NC


def select_kernel(count, here_ref, *refs):
    toks, grads, outs = refs[:count], refs[count : 2 * count], refs[2 * count :]
    y, z, c = here_ref[0], here_ref[1], here_ref[2]
    rows, width = grads[0].shape
    slots = NY * NC * CAP
    column = lax.broadcasted_iota(jnp.int32, (128, slots), 1)
    row = lax.broadcasted_iota(jnp.int32, (128, slots), 0)
    expert = jnp.zeros((128, slots), jnp.int32)
    slot = column
    for r in range(NY * NC):
        dy, dc = relative(r)
        number = ((y + dy) % NY) * (NZ * NC) + z * NC + (c + dc) % NC
        expert = jnp.where(column >= r * CAP, number, expert)
        slot = jnp.where(column >= r * CAP, column - r * CAP, slot)
    pick = (row == expert).astype(jnp.bfloat16)
    slot = slot.astype(jnp.float32)
    for i in range(count):
        place = toks[i][:, width:]
        spread = jnp.dot(place, pick, preferred_element_type=jnp.float32)
        chosen = (spread == slot).astype(jnp.float32).T.astype(jnp.bfloat16)
        for at in range(0, width, 512):
            for base, source in ((0, toks[i]), (width, grads[i])):
                taken = jnp.dot(
                    chosen, source[:, at : at + 512], preferred_element_type=jnp.float32
                )
                for r in range(NY * NC):
                    outs[r][i * CAP : (i + 1) * CAP, base + at : base + at + 512] = taken[
                        r * CAP : (r + 1) * CAP
                    ].astype(jnp.bfloat16)


def select(here, toks, grads):
    count = len(toks)
    rows, width = grads[0].shape
    return pl.pallas_call(
        functools.partial(select_kernel, count),
        out_shape=[jax.ShapeDtypeStruct((count * CAP, 2 * width), jnp.bfloat16)] * (NY * NC),
        in_specs=[pl.BlockSpec(memory_space=pltpu.SMEM)]
        + [pl.BlockSpec(memory_space=pltpu.VMEM)] * (2 * count),
        out_specs=[pl.BlockSpec(memory_space=pltpu.VMEM)] * (NY * NC),
        compiler_params=pltpu.CompilerParams(vmem_limit_bytes=VMEM),
        cost_estimate=pl.CostEstimate(
            flops=2 * 192 * 128 * 4096 * count, bytes_accessed=3 << 20, transcendentals=0
        ),
    )(here, *toks, *grads)


def expert_kernel(offsets, steps, here_ref, *refs):
    parts = NY * NC
    ins = refs[:parts]
    gate_ref, up_ref, down_ref, before_ref, out_ref, flat, total = refs[parts:]
    y, z, c = here_ref[0], here_ref[1], here_ref[2]
    rows, width = ins[0].shape[0], ins[0].shape[1] // 2
    step = pl.program_id(0)

    @pl.when(step == 0)
    def _():
        for r in range(parts):
            flat[r * rows : (r + 1) * rows, :] = ins[r][:, :width]

    gate_in = jnp.dot(flat[...], gate_ref[...], preferred_element_type=jnp.float32)
    up_in = jnp.dot(flat[...], up_ref[...], preferred_element_type=jnp.float32)
    hidden = (gate_in / (1.0 + jnp.exp(-gate_in)) * up_in).astype(jnp.bfloat16)
    term = jnp.dot(hidden, down_ref[...], preferred_element_type=jnp.float32)

    @pl.when(step == 0)
    def _():
        total[...] = term

    @pl.when(step > 0)
    def _():
        total[...] += term

    @pl.when(step == steps - 1)
    def _():
        out_ref[...] = before_ref[...]
        lane = lax.broadcasted_iota(jnp.int32, (CAP, 128), 1)
        row = lax.broadcasted_iota(jnp.int32, (CAP, 128), 0)
        for r in range(parts):
            dy, dc = relative(r)
            home = ((y + NY - dy) % NY) * NC + (c + NC - dc) % NC
            for i, offset in enumerate(offsets):
                at = r * rows + i * CAP
                made = total[at : at + CAP, :].astype(jnp.bfloat16).astype(jnp.float32)
                grad = ins[r][i * CAP : (i + 1) * CAP, width:].astype(jnp.float32)
                dots = jnp.sum(made * grad, axis=1, keepdims=True)
                line = jnp.sum(jnp.where(row == lane, dots, 0.0), axis=0, keepdims=True)
                out_ref[home, pl.ds((z + offset) % NZ, 1), :] = line


def expert(here, offsets, parts, gate_w, up_w, down_w, before):
    rows = parts[0].shape[0]
    width, inner = gate_w.shape
    tile = 256
    steps = inner // tile
    everything = len(parts) * rows
    whole = pl.BlockSpec((rows, 2 * width), lambda f: (0, 0))
    return pl.pallas_call(
        functools.partial(expert_kernel, offsets, steps),
        grid=(steps,),
        out_shape=jax.ShapeDtypeStruct(before.shape, jnp.float32),
        in_specs=[pl.BlockSpec(memory_space=pltpu.SMEM)]
        + [whole] * len(parts)
        + [
            pl.BlockSpec((width, tile), lambda f: (0, f)),
            pl.BlockSpec((width, tile), lambda f: (0, f)),
            pl.BlockSpec((tile, width), lambda f: (f, 0)),
            pl.BlockSpec(before.shape, lambda f: (0, 0, 0)),
        ],
        out_specs=pl.BlockSpec(before.shape, lambda f: (0, 0, 0)),
        scratch_shapes=[
            pltpu.VMEM((everything, width), jnp.bfloat16),
            pltpu.VMEM((everything, width), jnp.float32),
        ],
        compiler_params=pltpu.CompilerParams(vmem_limit_bytes=VMEM),
        cost_estimate=pl.CostEstimate(
            flops=6 * everything * width * inner,
            bytes_accessed=12 << 20,
            transcendentals=everything * inner,
        ),
    )(here, *parts, gate_w, up_w, down_w, before)


def shifted_y(array, r):
    dy, dc = relative(r)
    pairs = [
        (y * NC + c, ((y + dy) % NY) * NC + (c + dc) % NC) for y in range(NY) for c in range(NC)
    ]
    return lax.ppermute(array, ("y", "c"), pairs)


def shifted_z(array, dz):
    return lax.ppermute(array, "z", [(z, (z + dz) % NZ) for z in range(NZ)])


def sum_at_owner(array, axis):
    parts = array.reshape(NY * NZ * NC, -1, array.shape[1])
    arrived = lax.all_to_all(parts, axis, split_axis=0, concat_axis=0, tiled=True)
    return arrived.sum(axis=0)


def on_device(tokens, grad_out, router_weight, expert_index, w_gate, w_up, w_down):
    tok_rows, width = tokens.shape
    experts = router_weight.shape[1]
    here = jnp.stack([lax.axis_index(a) for a in ("y", "z", "c")]).astype(jnp.int32)
    placed = pl.pallas_call(
        place_kernel,
        out_shape=jax.ShapeDtypeStruct((tok_rows, width + 128), jnp.bfloat16),
        compiler_params=pltpu.CompilerParams(vmem_limit_bytes=VMEM),
    )(tokens, expert_index)

    up_t, up_g, down_t, down_g = [placed], [grad_out], [placed], [grad_out]
    for step in range(3):
        up_t.append(shifted_z(up_t[-1], 1))
        down_t.append(shifted_z(down_t[-1], -1))
        up_g.append(shifted_z(up_g[-1], 1))
        down_g.append(shifted_z(down_g[-1], -1))
    far_t, far_g = shifted_z(up_t[-1], 1), shifted_z(down_g[-1], -1)
    groups = [((0,), [placed], [grad_out])]
    for step in range(1, 4):
        groups.append(
            ((NZ - step, step), [up_t[step], down_t[step]], [up_g[step], down_g[step]])
        )
    groups.append(((4,), [far_t], [far_g]))

    products = jnp.zeros((NY * NC, NZ, 128), jnp.float32)
    arrived = []
    for offsets, toks, grads in groups:
        rows = select(here, toks, grads)
        arrived.append([rows[0]] + [shifted_y(rows[r], r) for r in range(1, NY * NC)])
    for (offsets, _, _), parts in zip(groups, arrived):
        products = expert(here, offsets, parts, w_gate[0], w_up[0], w_down[0], products)

    back = lax.all_to_all(products, ("y", "c"), 0, 0, tiled=True)
    back = lax.all_to_all(
        jnp.broadcast_to(back[None], (NZ, *back.shape)), "z", 0, 0, tiled=True
    )
    mine = lax.dynamic_index_in_dim(back, lax.axis_index("z"), 2, keepdims=False)
    mine = mine[..., :CAP].reshape(NZ, NY, NC, CAP).transpose(1, 0, 2, 3).reshape(experts, CAP)

    labels = jnp.arange(experts, dtype=jnp.int32)
    hits = expert_index[:, :, None] == labels
    masks = hits.astype(jnp.float32)
    place = placed[:, width : width + experts].astype(jnp.int32)
    wide = jnp.sum(
        jnp.where(place[:, :, None] == jnp.arange(CAP, dtype=jnp.int32), mine[None], 0.0), axis=2
    )
    gate_grad = jnp.sum(masks * wide[:, None, :], axis=2)
    logits = jnp.dot(tokens, router_weight, preferred_element_type=jnp.float32)
    chosen = jnp.sum(masks * logits[:, None, :], axis=2)
    weights = jnp.exp(chosen)
    gates = weights / jnp.sum(weights, axis=1, keepdims=True)
    mean_term = jnp.sum(gates * gate_grad, axis=1, keepdims=True)
    logit_grad = gates * (gate_grad - mean_term)
    dense = jnp.sum(logit_grad[:, :, None] * masks, axis=1)
    wide_tokens = tokens.astype(jnp.float32)
    part = sum_at_owner(jnp.dot(wide_tokens.T, dense), ("y", "z", "c"))
    everyone = lax.all_to_all(
        jnp.broadcast_to(part[None], (lax.axis_size("dp"), *part.shape)), "dp", 0, 0, tiled=True
    )
    return (gate_grad, jnp.sum(everyone, axis=0))


def solution(mesh):
    devices = mesh.devices.reshape(mesh.devices.shape[0], NY, NZ, NC)
    fine = Mesh(devices, ("dp", "y", "z", "c"))
    rows = P(("dp", "y", "z", "c"), None)
    own = P(("y", "z", "c"), None, None)
    return jax.shard_map(
        on_device,
        mesh=fine,
        in_specs=(rows, rows, P(), rows, own, own, own),
        out_specs=(rows, P(("y", "z", "c"), None)),
        check_vma=False,
    )
```

```python
import functools

import jax
import jax.numpy as jnp
from jax import lax
from jax.experimental import pallas as pl
from jax.experimental.pallas import tpu as pltpu
from jax.sharding import Mesh, PartitionSpec as P


NY, NZ, NC = 4, 8, 2
CAP = 24
PACK, STRIDE = 4, 32
VMEM = 48 * 1024 * 1024


def place_kernel(tok_ref, idx_ref, out_ref):
    rows, width = tok_ref.shape
    out_ref[:, :width] = tok_ref[...]
    lane = lax.broadcasted_iota(jnp.int32, (rows, 128), 1)
    hit = jnp.zeros((rows, 128), jnp.float32)
    for k in range(idx_ref.shape[1]):
        hit = hit + (idx_ref[:, k : k + 1] == lane).astype(jnp.float32)
    earlier = lax.broadcasted_iota(jnp.int32, (rows, rows), 0) > lax.broadcasted_iota(
        jnp.int32, (rows, rows), 1
    )
    before = jnp.dot(
        earlier.astype(jnp.bfloat16),
        hit.astype(jnp.bfloat16),
        preferred_element_type=jnp.float32,
    )
    out_ref[:, width:] = jnp.where(hit > 0.0, before, -1.0).astype(jnp.bfloat16)


def relative(r):
    return r // NC, r % NC


def select_kernel(count, here_ref, *refs):
    toks, grads, outs = refs[:count], refs[count : 2 * count], refs[2 * count :]
    y, z, c = here_ref[0], here_ref[1], here_ref[2]
    _, width = grads[0].shape
    slots = NY * NC * CAP
    column = lax.broadcasted_iota(jnp.int32, (128, slots), 1)
    row = lax.broadcasted_iota(jnp.int32, (128, slots), 0)
    expert = jnp.zeros((128, slots), jnp.int32)
    slot = column
    for r in range(NY * NC):
        dy, dc = relative(r)
        number = ((y + dy) % NY) * (NZ * NC) + z * NC + (c + dc) % NC
        expert = jnp.where(column >= r * CAP, number, expert)
        slot = jnp.where(column >= r * CAP, column - r * CAP, slot)
    pick = (row == expert).astype(jnp.bfloat16)
    slot = slot.astype(jnp.float32)
    for i in range(count):
        place = toks[i][:, width:]
        spread = jnp.dot(place, pick, preferred_element_type=jnp.float32)
        chosen = (spread == slot).astype(jnp.float32).T.astype(jnp.bfloat16)
        for at in range(0, width, 512):
            for base, source in ((0, toks[i]), (width, grads[i])):
                taken = jnp.dot(
                    chosen, source[:, at : at + 512], preferred_element_type=jnp.float32
                )
                for r in range(NY * NC):
                    outs[r][i * CAP : (i + 1) * CAP, base + at : base + at + 512] = taken[
                        r * CAP : (r + 1) * CAP
                    ].astype(jnp.bfloat16)


def select(here, toks, grads):
    count = len(toks)
    _, width = grads[0].shape
    return pl.pallas_call(
        functools.partial(select_kernel, count),
        out_shape=[jax.ShapeDtypeStruct((count * CAP, 2 * width), jnp.bfloat16)] * (NY * NC),
        in_specs=[pl.BlockSpec(memory_space=pltpu.SMEM)]
        + [pl.BlockSpec(memory_space=pltpu.VMEM)] * (2 * count),
        out_specs=[pl.BlockSpec(memory_space=pltpu.VMEM)] * (NY * NC),
        compiler_params=pltpu.CompilerParams(vmem_limit_bytes=VMEM),
        cost_estimate=pl.CostEstimate(
            flops=2 * 192 * 128 * 4096 * count, bytes_accessed=3 << 20, transcendentals=0
        ),
    )(here, *toks, *grads)


def expert_kernel(offsets, steps, here_ref, *refs):
    parts = NY * NC
    ins = refs[:parts]
    gate_ref, up_ref, down_ref, before_ref, out_ref, flat, total = refs[parts:]
    y, z, c = here_ref[0], here_ref[1], here_ref[2]
    rows, width = ins[0].shape[0], ins[0].shape[1] // 2
    step = pl.program_id(0)

    @pl.when(step == 0)
    def _():
        for r in range(parts):
            flat[r * rows : (r + 1) * rows, :] = ins[r][:, :width]

    gate_in = jnp.dot(flat[...], gate_ref[...], preferred_element_type=jnp.float32)
    up_in = jnp.dot(flat[...], up_ref[...], preferred_element_type=jnp.float32)
    hidden = (gate_in / (1.0 + jnp.exp(-gate_in)) * up_in).astype(jnp.bfloat16)
    term = jnp.dot(hidden, down_ref[...], preferred_element_type=jnp.float32)

    @pl.when(step == 0)
    def _():
        total[...] = term

    @pl.when(step > 0)
    def _():
        total[...] += term

    @pl.when(step == steps - 1)
    def _():
        out_ref[...] = before_ref[...]
        lane = lax.broadcasted_iota(jnp.int32, (CAP, 128), 1)
        row = lax.broadcasted_iota(jnp.int32, (CAP, 128), 0)
        for r in range(parts):
            dy, dc = relative(r)
            home = ((y + NY - dy) % NY) * NC + (c + NC - dc) % NC
            for i, offset in enumerate(offsets):
                at = r * rows + i * CAP
                made = total[at : at + CAP, :].astype(jnp.bfloat16).astype(jnp.float32)
                grad = ins[r][i * CAP : (i + 1) * CAP, width:].astype(jnp.float32)
                dots = jnp.sum(made * grad, axis=1, keepdims=True)
                source = (z + offset) % NZ
                at_lane = row + (source % PACK) * STRIDE
                line = jnp.sum(jnp.where(at_lane == lane, dots, 0.0), axis=0, keepdims=True)
                out_ref[home, pl.ds(source // PACK, 1), :] += line


def expert(here, offsets, parts, gate_w, up_w, down_w, before):
    rows = parts[0].shape[0]
    width, inner = gate_w.shape
    tile = 256
    steps = inner // tile
    everything = len(parts) * rows
    whole = pl.BlockSpec((rows, 2 * width), lambda f: (0, 0))
    return pl.pallas_call(
        functools.partial(expert_kernel, offsets, steps),
        grid=(steps,),
        out_shape=jax.ShapeDtypeStruct(before.shape, jnp.float32),
        in_specs=[pl.BlockSpec(memory_space=pltpu.SMEM)]
        + [whole] * len(parts)
        + [
            pl.BlockSpec((width, tile), lambda f: (0, f)),
            pl.BlockSpec((width, tile), lambda f: (0, f)),
            pl.BlockSpec((tile, width), lambda f: (f, 0)),
            pl.BlockSpec(before.shape, lambda f: (0, 0, 0)),
        ],
        out_specs=pl.BlockSpec(before.shape, lambda f: (0, 0, 0)),
        scratch_shapes=[
            pltpu.VMEM((everything, width), jnp.bfloat16),
            pltpu.VMEM((everything, width), jnp.float32),
        ],
        compiler_params=pltpu.CompilerParams(vmem_limit_bytes=VMEM),
        cost_estimate=pl.CostEstimate(
            flops=6 * everything * width * inner,
            bytes_accessed=12 << 20,
            transcendentals=everything * inner,
        ),
    )(here, *parts, gate_w, up_w, down_w, before)


def shifted_y(array, r):
    dy, dc = relative(r)
    pairs = [
        (y * NC + c, ((y + dy) % NY) * NC + (c + dc) % NC) for y in range(NY) for c in range(NC)
    ]
    return lax.ppermute(array, ("y", "c"), pairs)


def shifted_z(array, dz):
    return lax.ppermute(array, "z", [(z, (z + dz) % NZ) for z in range(NZ)])


def regroup():
    lane = lax.broadcasted_iota(jnp.int32, (128, 64), 1)
    row = lax.broadcasted_iota(jnp.int32, (128, 64), 0)
    return (row == natural(lane)).astype(jnp.bfloat16)


def natural(lane):
    inner = NY * NC
    return (lane % inner) // NC * (NZ * NC) + lane // inner * NC + lane % NC


def side_kernel(here_ref, *refs):
    slices, router_ref, gates_ref, place_ref, feats_ref = refs[:NZ], *refs[NZ:]
    z = here_ref[1]
    rows = slices[0].shape[0]
    width = router_ref.shape[0]
    order = regroup()
    router = jnp.dot(
        router_ref[...], order[:64], preferred_element_type=jnp.float32
    ).astype(jnp.bfloat16)
    for j in range(NZ):
        source = (z + j) % NZ
        place = jnp.dot(slices[j][:, width:], order, preferred_element_type=jnp.float32)
        logits = jnp.dot(slices[j][:, :width], router, preferred_element_type=jnp.float32)
        hit = place >= 0.0
        weights = jnp.where(hit, jnp.exp(jnp.where(hit, logits, 0.0)), 0.0)
        gates_ref[source] = weights / jnp.sum(weights, axis=1, keepdims=True)
        place_ref[source] = place
        at = pl.multiple_of(source * rows, rows)
        for y in range(NY):
            col = pl.multiple_of(y * (width // NY) + (z // 2) * 128, 128)
            feats_ref[pl.ds(at, rows), y * 128 : (y + 1) * 128] = slices[j][:, pl.ds(col, 128)]


def side(here, slices, router_weight):
    rows, experts = slices[0].shape[0], router_weight.shape[1]
    vmem = pl.BlockSpec(memory_space=pltpu.VMEM)
    return pl.pallas_call(
        side_kernel,
        out_shape=[
            jax.ShapeDtypeStruct((NZ, rows, experts), jnp.float32),
            jax.ShapeDtypeStruct((NZ, rows, experts), jnp.float32),
            jax.ShapeDtypeStruct((NZ * rows, NY * 128), jnp.bfloat16),
        ],
        in_specs=[pl.BlockSpec(memory_space=pltpu.SMEM)] + [vmem] * (NZ + 1),
        out_specs=[vmem] * 3,
        compiler_params=pltpu.CompilerParams(vmem_limit_bytes=VMEM),
        cost_estimate=pl.CostEstimate(
            flops=2 * NZ * rows * 2048 * 256, bytes_accessed=6 << 20, transcendentals=NZ * rows * 64
        ),
    )(here, *slices, router_weight)


def finish_kernel(here_ref, back_ref, gates_ref, place_ref, feats_ref, idx_ref, grad_ref, part_ref, wide_ref, dense_ref, sum_ref):
    z = here_ref[1]
    rows, experts = gates_ref.shape[1:]
    for a in range(NZ // PACK):
        table = back_ref[:, a, :].T
        for b in range(PACK):
            source = a * PACK + b
            place = place_ref[source]
            wide = jnp.zeros((rows, experts), jnp.float32)
            for s in range(CAP):
                line = table[b * STRIDE + s : b * STRIDE + s + 1, :]
                wide = jnp.where(place == float(s), line, wide)
            wide_ref[source] = wide
            gates = gates_ref[source]
            mean = jnp.sum(gates * wide, axis=1, keepdims=True)
            dense_ref[source * rows : (source + 1) * rows, :] = (gates * (wide - mean)).astype(
                jnp.bfloat16
            )
    back = regroup()[:experts]
    dense = lax.dot_general(
        dense_ref[...], back, (((1,), (1,)), ((), ())), preferred_element_type=jnp.float32
    ).astype(jnp.bfloat16)
    part = lax.dot_general(
        dense, feats_ref[...], (((0,), (0,)), ((), ())), preferred_element_type=jnp.float32
    )
    sum_ref[...] = part.T
    half = 16
    for y in range(NY):
        for c in range(NC):
            at = pl.multiple_of(y * 128 + (z % 2) * 64 + c * 32, 32)
            for copy in range(part_ref.shape[0]):
                part_ref[copy, y * NC + c, :, :experts] = sum_ref[pl.ds(at, half), :]
                part_ref[copy, y * NC + c, :, experts:] = sum_ref[pl.ds(at + half, half), :]
    own = wide_ref[z]
    number = natural(lax.broadcasted_iota(jnp.int32, (rows, experts), 1))
    lane = lax.broadcasted_iota(jnp.int32, grad_ref.shape, 1)
    out = jnp.zeros(grad_ref.shape, jnp.float32)
    for k in range(grad_ref.shape[1]):
        here_k = idx_ref[:, k : k + 1] == number
        value = jnp.sum(jnp.where(here_k, own, 0.0), axis=1, keepdims=True)
        out = jnp.where(lane == k, value, out)
    grad_ref[...] = out


def finish(here, back, gates, place, feats, expert_index, copies):
    rows, top = expert_index.shape
    experts = gates.shape[2]
    vmem = pl.BlockSpec(memory_space=pltpu.VMEM)
    return pl.pallas_call(
        finish_kernel,
        out_shape=[
            jax.ShapeDtypeStruct((rows, top), jnp.float32),
            jax.ShapeDtypeStruct((copies, NY * NC, 16, 2 * experts), jnp.float32),
        ],
        in_specs=[pl.BlockSpec(memory_space=pltpu.SMEM)] + [vmem] * 5,
        out_specs=[vmem] * 2,
        scratch_shapes=[
            pltpu.VMEM((NZ, rows, experts), jnp.float32),
            pltpu.VMEM((NZ * rows, experts), jnp.bfloat16),
            pltpu.VMEM((NY * 128, experts), jnp.float32),
        ],
        compiler_params=pltpu.CompilerParams(vmem_limit_bytes=VMEM),
        cost_estimate=pl.CostEstimate(flops=1 << 28, bytes_accessed=3 << 20, transcendentals=0),
    )(here, back, gates, place, feats, expert_index)


def sum_kernel(parts_ref, out_ref):
    total = parts_ref[0]
    for i in range(1, parts_ref.shape[0]):
        total = total + parts_ref[i]
    half, lanes = total.shape
    out_ref[:half, :] = total[:, : lanes // 2]
    out_ref[half:, :] = total[:, lanes // 2 :]


def on_device(tokens, grad_out, router_weight, expert_index, w_gate, w_up, w_down):
    tok_rows, width = tokens.shape
    experts = router_weight.shape[1]
    here = jnp.stack([lax.axis_index(a) for a in ("y", "z", "c")]).astype(jnp.int32)
    placed = pl.pallas_call(
        place_kernel,
        out_shape=jax.ShapeDtypeStruct((tok_rows, width + 128), jnp.bfloat16),
        compiler_params=pltpu.CompilerParams(vmem_limit_bytes=VMEM),
    )(tokens, expert_index)

    offsets, arrived, slices = [], [], {}
    ups, downs = (placed, grad_out), (placed, grad_out)
    for step in range(NZ // 2 + 1):
        if step == 0:
            slices[0] = placed
            stops, toks, grads = (0,), [placed], [grad_out]
        elif step < NZ // 2:
            slices[NZ - step], slices[step] = ups[0], downs[0]
            stops = (NZ - step, step)
            toks, grads = [ups[0], downs[0]], [ups[1], downs[1]]
        else:
            slices[step] = ups[0]
            stops, toks, grads = (step,), [ups[0]], [downs[1]]
        if step < NZ // 2 - 1:
            ups_next = tuple(shifted_z(a, 1) for a in ups)
            downs_next = tuple(shifted_z(a, -1) for a in downs)
        elif step == NZ // 2 - 1:
            ups_next = (shifted_z(ups[0], 1), None)
            downs_next = (None, shifted_z(downs[1], -1))
        rows = select(here, toks, grads)
        ups, downs = ups_next, downs_next
        offsets.append(stops)
        arrived.append([rows[0]] + [shifted_y(rows[r], r) for r in range(1, NY * NC)])

    products = jnp.zeros((NY * NC, NZ // PACK, 128), jnp.float32)
    for stops, parts in zip(offsets, arrived):
        products = expert(here, stops, parts, w_gate[0], w_up[0], w_down[0], products)
    gates, place, feats = side(here, [slices[j] for j in range(NZ)], router_weight)

    back = lax.all_to_all(products, ("y", "c"), 0, 0, tiled=True)
    back = lax.all_to_all(
        jnp.broadcast_to(back[None], (NZ, *back.shape)), "z", 0, 0, tiled=True
    )
    copies = lax.axis_size("dp")
    gate_grad, part = finish(
        here, back.reshape(experts, NZ // PACK, 128), gates, place, feats, expert_index, copies
    )
    parts = lax.all_to_all(
        part.reshape(copies * NY * NC, 16, 2 * experts), ("dp", "y", "c"), 0, 0, tiled=True
    )
    router_grad = pl.pallas_call(
        sum_kernel, out_shape=jax.ShapeDtypeStruct((32, experts), jnp.float32)
    )(parts)
    return (gate_grad, router_grad)


def solution(mesh):
    devices = mesh.devices.reshape(mesh.devices.shape[0], NY, NZ, NC)
    fine = Mesh(devices, ("dp", "y", "z", "c"))
    rows = P(("dp", "y", "z", "c"), None)
    own = P(("y", "z", "c"), None, None)

    return jax.shard_map(
        on_device,
        mesh=fine,
        in_specs=(rows, rows, P(), rows, own, own, own),
        out_specs=(rows, P(("y", "z", "c"), None)),
        check_vma=False,
    )
```

```python
import functools

import jax
import jax.numpy as jnp
import numpy as np
from jax import lax
from jax.experimental import pallas as pl
from jax.experimental.pallas import tpu as pltpu
from jax.sharding import Mesh, PartitionSpec as P


NY, NZ, NC = 4, 8, 2
CAP = 24
PACK, STRIDE = 4, 32
VMEM = 48 * 1024 * 1024


def params():
    return pltpu.CompilerParams(vmem_limit_bytes=VMEM)


def in_vmem(count):
    return [pl.BlockSpec(memory_space=pltpu.VMEM)] * count


def in_smem():
    return [pl.BlockSpec(memory_space=pltpu.SMEM)]


def pack_kernel(tok_ref, grad_ref, idx_ref, out_ref):
    rows, width = tok_ref.shape
    out_ref[:, :width] = tok_ref[...]
    out_ref[:, width : 2 * width] = grad_ref[...]
    lane = lax.broadcasted_iota(jnp.int32, (rows, 128), 1)
    hit = jnp.zeros((rows, 128), jnp.float32)
    for k in range(idx_ref.shape[1]):
        hit = hit + (idx_ref[:, k : k + 1] == lane).astype(jnp.float32)
    earlier = lax.broadcasted_iota(jnp.int32, (rows, rows), 0) > lax.broadcasted_iota(
        jnp.int32, (rows, rows), 1
    )
    before = jnp.dot(
        earlier.astype(jnp.bfloat16),
        hit.astype(jnp.bfloat16),
        preferred_element_type=jnp.float32,
    )
    out_ref[:, 2 * width :] = jnp.where(hit > 0.0, before, -1.0).astype(jnp.bfloat16)


def pick_kernel(count, here_ref, *refs):
    slices, outs, chosen_ref = refs[:count], refs[count:-1], refs[-1]
    y, z, c = here_ref[0], here_ref[1], here_ref[2]
    width = outs[0].shape[1]
    slots = NY * CAP
    column = lax.broadcasted_iota(jnp.int32, (128, slots), 1)
    row = lax.broadcasted_iota(jnp.int32, (128, slots), 0)
    expert = jnp.zeros((128, slots), jnp.int32)
    slot = column
    for dy in range(NY):
        number = ((y + dy) % NY) * (NZ * NC) + z * NC + c
        expert = jnp.where(column >= dy * CAP, number, expert)
        slot = jnp.where(column >= dy * CAP, column - dy * CAP, slot)
    choose = (row == expert).astype(jnp.bfloat16)
    slot = slot.astype(jnp.float32)
    for i in range(count):
        place = slices[i][:, width:]
        spread = jnp.dot(place, choose, preferred_element_type=jnp.float32)
        chosen_ref[i] = (spread == slot).astype(jnp.float32).T.astype(jnp.bfloat16)

    tile = 1024

    @pl.loop(0, width // tile)
    def _(step):
        cols = pl.ds(pl.multiple_of(step * tile, tile), tile)
        for i in range(count):
            taken = jnp.dot(
                chosen_ref[i], slices[i][:, cols], preferred_element_type=jnp.float32
            )
            for dy in range(NY):
                outs[dy][i * CAP : (i + 1) * CAP, cols] = taken[
                    dy * CAP : (dy + 1) * CAP
                ].astype(jnp.bfloat16)


def pick(here, slices):
    count = len(slices)
    rows, width = slices[0].shape[0], slices[0].shape[1] - 128
    return pl.pallas_call(
        functools.partial(pick_kernel, count),
        out_shape=[jax.ShapeDtypeStruct((count * CAP, width), jnp.bfloat16)] * NY,
        in_specs=in_smem() + in_vmem(count),
        out_specs=in_vmem(NY),
        scratch_shapes=[pltpu.VMEM((count, NY * CAP, rows), jnp.bfloat16)],
        compiler_params=params(),
        cost_estimate=pl.CostEstimate(
            flops=2 * 96 * 128 * 4096 * count, bytes_accessed=2 * count << 20, transcendentals=0
        ),
    )(here, *slices)


def expert_kernel(steps, chunk, table_ref, *refs):
    (*ins, gate_ref, up_ref, down_ref, before_ref, out_ref, toks, grads, total) = refs
    rows, width = toks.shape
    step = pl.program_id(0)

    @pl.when(step == 0)
    def _():
        at = 0
        for part in ins:
            toks[at : at + part.shape[0], :] = part[:, :width]
            grads[at : at + part.shape[0], :] = part[:, width:]
            at += part.shape[0]

    @pl.loop(0, rows // chunk)
    def _(i):
        own = pl.ds(pl.multiple_of(i * chunk, chunk), chunk)
        x = toks[own, :]
        gate_in = jnp.dot(x, gate_ref[...], preferred_element_type=jnp.float32)
        up_in = jnp.dot(x, up_ref[...], preferred_element_type=jnp.float32)
        hidden = (gate_in / (1.0 + jnp.exp(-gate_in)) * up_in).astype(jnp.bfloat16)
        term = jnp.dot(hidden, down_ref[...], preferred_element_type=jnp.float32)

        @pl.when(step == 0)
        def _():
            total[own, :] = term

        @pl.when(step > 0)
        def _():
            total[own, :] += term

    @pl.when(step == steps - 1)
    def _():
        out_ref[...] = before_ref[...]
        lane = lax.broadcasted_iota(jnp.int32, (CAP, 128), 1)
        row = lax.broadcasted_iota(jnp.int32, (CAP, 128), 0)

        @pl.loop(0, rows // (2 * CAP))
        def _(pair):
            first = pl.multiple_of(pair * (2 * CAP), 2 * CAP)
            made = total[pl.ds(first, 2 * CAP), :].astype(jnp.bfloat16).astype(jnp.float32)
            grad = grads[pl.ds(first, 2 * CAP), :].astype(jnp.float32)
            dots = jnp.sum(made * grad, axis=1, keepdims=True)
            for half in range(2):
                home = table_ref[0, 2 * pair + half]
                source = table_ref[1, 2 * pair + half]
                mine = dots[half * CAP : (half + 1) * CAP]
                at_lane = row + (source % PACK) * STRIDE
                line = jnp.sum(jnp.where(at_lane == lane, mine, 0.0), axis=0, keepdims=True)
                out_ref[home, pl.ds(source // PACK, 1), :] += line


def expert(table, parts, gate_w, up_w, down_w, before):
    width, inner = gate_w.shape
    tile = 256
    steps = inner // tile
    rows = sum(part.shape[0] for part in parts)
    chunk = rows if rows <= 384 else rows // 2
    return pl.pallas_call(
        functools.partial(expert_kernel, steps, chunk),
        grid=(steps,),
        out_shape=jax.ShapeDtypeStruct(before.shape, jnp.float32),
        in_specs=in_smem()
        + [pl.BlockSpec(part.shape, lambda f: (0, 0)) for part in parts]
        + [
            pl.BlockSpec((width, tile), lambda f: (0, f)),
            pl.BlockSpec((width, tile), lambda f: (0, f)),
            pl.BlockSpec((tile, width), lambda f: (f, 0)),
            pl.BlockSpec(before.shape, lambda f: (0, 0, 0)),
        ],
        out_specs=pl.BlockSpec(before.shape, lambda f: (0, 0, 0)),
        scratch_shapes=[
            pltpu.VMEM((rows, width), jnp.bfloat16),
            pltpu.VMEM((rows, width), jnp.bfloat16),
            pltpu.VMEM((rows, width), jnp.float32),
        ],
        compiler_params=params(),
        cost_estimate=pl.CostEstimate(
            flops=6 * rows * width * inner, bytes_accessed=12 << 20, transcendentals=rows * inner
        ),
    )(table, *parts, gate_w, up_w, down_w, before)


def side_kernel(here_ref, *refs):
    slices, router_ref, gates_ref, place_ref, feats_ref = refs[:NZ], *refs[NZ:]
    z = here_ref[1]
    rows = slices[0].shape[0]
    width, experts = router_ref.shape
    router = router_ref[...]
    for j in range(NZ):
        source = (z + j) % NZ
        place = slices[j][:, 2 * width :].astype(jnp.float32)[:, :experts]
        logits = jnp.dot(slices[j][:, :width], router, preferred_element_type=jnp.float32)
        hit = place >= 0.0
        weights = jnp.where(hit, jnp.exp(jnp.where(hit, logits, 0.0)), 0.0)
        gates_ref[source] = weights / jnp.sum(weights, axis=1, keepdims=True)
        place_ref[source] = place
        at = pl.multiple_of(source * rows, rows)
        for y in range(NY):
            col = pl.multiple_of(y * (width // NY) + (z // 2) * 128, 128)
            feats_ref[pl.ds(at, rows), y * 128 : (y + 1) * 128] = slices[j][:, pl.ds(col, 128)]


def side(here, slices, router_weight):
    rows, experts = slices[0].shape[0], router_weight.shape[1]
    return pl.pallas_call(
        side_kernel,
        out_shape=[
            jax.ShapeDtypeStruct((NZ, rows, experts), jnp.float32),
            jax.ShapeDtypeStruct((NZ, rows, experts), jnp.float32),
            jax.ShapeDtypeStruct((NZ * rows, NY * 128), jnp.bfloat16),
        ],
        in_specs=in_smem() + in_vmem(NZ + 1),
        out_specs=in_vmem(3),
        compiler_params=params(),
        cost_estimate=pl.CostEstimate(
            flops=2 * NZ * rows * 2048 * 256, bytes_accessed=6 << 20, transcendentals=NZ * rows * 64
        ),
    )(here, *slices, router_weight)


def finish_kernel(
    here_ref, back_ref, gates_ref, place_ref, feats_ref, idx_ref,
    grad_ref, part_ref, table_ref, wide_ref, dense_ref, sum_ref,
):
    z = here_ref[1]
    rows, experts = gates_ref.shape[1:]
    for a in range(NZ // PACK):
        table_ref[a * 128 : (a + 1) * 128, :] = back_ref[:, a, :].T

    @pl.loop(0, NZ)
    def _(source):
        place = place_ref[source]
        lines = table_ref[pl.ds(pl.multiple_of(source * STRIDE, STRIDE), STRIDE), :]
        wide = jnp.zeros((rows, experts), jnp.float32)
        for s in range(CAP):
            wide = jnp.where(place == float(s), lines[s : s + 1, :], wide)
        wide_ref[source] = wide
        gates = gates_ref[source]
        mean = jnp.sum(gates * wide, axis=1, keepdims=True)
        at = pl.multiple_of(source * rows, rows)
        dense_ref[pl.ds(at, rows), :] = (gates * (wide - mean)).astype(jnp.bfloat16)

    part = lax.dot_general(
        dense_ref[...],
        feats_ref[...],
        (((0,), (0,)), ((), ())),
        preferred_element_type=jnp.float32,
    )
    sum_ref[...] = part.T
    half = 16
    for y in range(NY):
        for c in range(NC):
            at = pl.multiple_of(y * 128 + (z % 2) * 64 + c * 32, 32)
            for copy in range(part_ref.shape[0]):
                part_ref[copy, y * NC + c, :, :experts] = sum_ref[pl.ds(at, half), :]
                part_ref[copy, y * NC + c, :, experts:] = sum_ref[pl.ds(at + half, half), :]
    own = wide_ref[z]
    number = lax.broadcasted_iota(jnp.int32, (rows, experts), 1)
    lane = lax.broadcasted_iota(jnp.int32, grad_ref.shape, 1)
    out = jnp.zeros(grad_ref.shape, jnp.float32)
    for k in range(grad_ref.shape[1]):
        here_k = idx_ref[:, k : k + 1] == number
        value = jnp.sum(jnp.where(here_k, own, 0.0), axis=1, keepdims=True)
        out = jnp.where(lane == k, value, out)
    grad_ref[...] = out


def finish(here, back, gates, place, feats, expert_index, copies):
    rows, top = expert_index.shape
    experts = gates.shape[2]
    return pl.pallas_call(
        finish_kernel,
        out_shape=[
            jax.ShapeDtypeStruct((rows, top), jnp.float32),
            jax.ShapeDtypeStruct((copies, NY * NC, 16, 2 * experts), jnp.float32),
        ],
        in_specs=in_smem() + in_vmem(5),
        out_specs=in_vmem(2),
        scratch_shapes=[
            pltpu.VMEM((NZ * STRIDE, experts), jnp.float32),
            pltpu.VMEM((NZ, rows, experts), jnp.float32),
            pltpu.VMEM((NZ * rows, experts), jnp.bfloat16),
            pltpu.VMEM((NY * 128, experts), jnp.float32),
        ],
        compiler_params=params(),
        cost_estimate=pl.CostEstimate(flops=1 << 28, bytes_accessed=3 << 20, transcendentals=0),
    )(here, back, gates, place, feats, expert_index)


def sum_kernel(parts_ref, out_ref):
    total = parts_ref[0]
    for i in range(1, parts_ref.shape[0]):
        total = total + parts_ref[i]
    half, lanes = total.shape
    out_ref[:half, :] = total[:, : lanes // 2]
    out_ref[half:, :] = total[:, lanes // 2 :]


def shifted(array, axis, by):
    size = lax.axis_size(axis)
    return lax.ppermute(array, axis, [(i, (i + by) % size) for i in range(size)])


def on_device(tokens, grad_out, router_weight, expert_index, w_gate, w_up, w_down):
    tok_rows, width = tokens.shape
    experts = router_weight.shape[1]
    y, z, c = (lax.axis_index(a) for a in ("y", "z", "c"))
    here = jnp.stack([y, z, c]).astype(jnp.int32)
    packed = pl.pallas_call(
        pack_kernel,
        out_shape=jax.ShapeDtypeStruct((tok_rows, 2 * width + 128), jnp.bfloat16),
        compiler_params=params(),
    )(tokens, grad_out, expert_index)

    last = NZ // 2
    ups, downs = {0: packed}, {0: packed}
    for step in range(1, last + 1):
        ups[step] = shifted(ups[step - 1], "z", 1)
        if step < last:
            downs[step] = shifted(downs[step - 1], "z", -1)
    stops, arrived = [], []
    for step in range(last + 1):
        if step == 0 or step == last:
            stops.append((step,))
            slices = [ups[step]]
        else:
            stops.append((NZ - step, step))
            slices = [ups[step], downs[step]]
        slices = slices + [shifted(a, "c", 1) for a in slices]
        rows = pick(here, slices)
        arrived.append([rows[0]] + [shifted(rows[dy], "y", dy) for dy in range(1, NY)])

    products = jnp.zeros((NY * NC, NZ // PACK, 128), jnp.float32)
    for steps in ((0, 1), (2,), (3,), (4,)):
        parts, table = [], []
        for step in steps:
            for dy in range(NY):
                parts.append(arrived[step][dy])
                for core in range(NC):
                    for offset in stops[step]:
                        table.append((dy, core, offset))
        dys, cores, offsets = np.array(table, np.int32).T
        homes = jnp.stack([(y + NY - dys) % NY * NC + (c + cores) % NC, (z + offsets) % NZ])
        products = expert(homes, parts, w_gate[0], w_up[0], w_down[0], products)
    columns = [ups[0]] + [downs[j] for j in range(1, last)] + [ups[last]]
    columns += [ups[j] for j in range(last - 1, 0, -1)]
    gates, place, feats = side(here, columns, router_weight)

    back = products.reshape(NY, 1, NC, NZ // PACK, 128)
    back = jnp.broadcast_to(back, (NY, NZ, NC, NZ // PACK, 128)).reshape(experts, NZ // PACK, 128)
    back = lax.all_to_all(back, ("y", "z", "c"), 0, 0, tiled=True)
    copies = lax.axis_size("dp")
    gate_grad, part = finish(here, back, gates, place, feats, expert_index, copies)
    parts = lax.all_to_all(
        part.reshape(copies * NY * NC, 16, 2 * experts), ("dp", "y", "c"), 0, 0, tiled=True
    )
    router_grad = pl.pallas_call(
        sum_kernel, out_shape=jax.ShapeDtypeStruct((32, experts), jnp.float32)
    )(parts)
    return (gate_grad, router_grad)


def solution(mesh):
    devices = mesh.devices.reshape(mesh.devices.shape[0], NY, NZ, NC)
    fine = Mesh(devices, ("dp", "y", "z", "c"))
    rows = P(("dp", "y", "z", "c"), None)
    own = P(("y", "z", "c"), None, None)

    return jax.shard_map(
        on_device,
        mesh=fine,
        in_specs=(rows, rows, P(), rows, own, own, own),
        out_specs=(rows, P(("y", "z", "c"), None)),
        check_vma=False,
    )
```

```python
import functools

import jax
import jax.numpy as jnp
import numpy as np
from jax import lax
from jax.experimental import pallas as pl
from jax.experimental.pallas import tpu as pltpu
from jax.sharding import Mesh, PartitionSpec as P


NY, NZ, NC = 4, 8, 2
CAP = 24
PACK, STRIDE = 4, 32
VMEM = 32 * 1024 * 1024


def params():
    return pltpu.CompilerParams(vmem_limit_bytes=VMEM)


def in_vmem(count):
    return [pl.BlockSpec(memory_space=pltpu.VMEM)] * count


def in_hbm(array):
    return pltpu.with_memory_space_constraint(array, pltpu.HBM)


def in_smem():
    return [pl.BlockSpec(memory_space=pltpu.SMEM)]


def pack_kernel(tok_ref, grad_ref, idx_ref, out_ref):
    rows, width = tok_ref.shape
    out_ref[:, :width] = tok_ref[...]
    out_ref[:, width : 2 * width] = grad_ref[...]
    label = lax.broadcasted_iota(jnp.int32, (128, rows), 0)
    hit = jnp.zeros((128, rows), jnp.float32)
    for k in range(idx_ref.shape[0]):
        hit = hit + (idx_ref[k : k + 1, :] == label).astype(jnp.float32)
    hit = hit.T
    earlier = lax.broadcasted_iota(jnp.int32, (rows, rows), 0) > lax.broadcasted_iota(
        jnp.int32, (rows, rows), 1
    )
    before = jnp.dot(
        earlier.astype(jnp.bfloat16),
        hit.astype(jnp.bfloat16),
        preferred_element_type=jnp.float32,
    )
    out_ref[:, 2 * width :] = jnp.where(hit > 0.0, before, -1.0).astype(jnp.bfloat16)


def pick_kernel(count, here_ref, *refs):
    slices, outs, chosen_ref = refs[:count], refs[count:-1], refs[-1]
    y, z, c = here_ref[0], here_ref[1], here_ref[2]
    width = outs[0].shape[1]
    slots = NY * CAP
    column = lax.broadcasted_iota(jnp.int32, (128, slots), 1)
    row = lax.broadcasted_iota(jnp.int32, (128, slots), 0)
    expert = jnp.zeros((128, slots), jnp.int32)
    slot = column
    for dy in range(NY):
        number = ((y + dy) % NY) * (NZ * NC) + z * NC + c
        expert = jnp.where(column >= dy * CAP, number, expert)
        slot = jnp.where(column >= dy * CAP, column - dy * CAP, slot)
    choose = (row == expert).astype(jnp.bfloat16)
    slot = slot.astype(jnp.float32)
    for i in range(count):
        place = slices[i][:, width:]
        spread = jnp.dot(place, choose, preferred_element_type=jnp.float32)
        chosen_ref[i] = (spread == slot).astype(jnp.float32).T.astype(jnp.bfloat16)

    tile = 1024

    @pl.loop(0, width // tile)
    def _(step):
        cols = pl.ds(pl.multiple_of(step * tile, tile), tile)
        for i in range(0, count, 2):
            taken = [
                jnp.dot(chosen_ref[j], slices[j][:, cols], preferred_element_type=jnp.float32)
                for j in (i, i + 1)
            ]
            for dy in range(NY):
                both = [t[dy * CAP : (dy + 1) * CAP] for t in taken]
                outs[dy][i * CAP : (i + 2) * CAP, cols] = jnp.concatenate(both, axis=0).astype(
                    jnp.bfloat16
                )


def pick(here, slices):
    count = len(slices)
    rows, width = slices[0].shape[0], slices[0].shape[1] - 128
    return pl.pallas_call(
        functools.partial(pick_kernel, count),
        out_shape=[pltpu.HBM((count * CAP, width), jnp.bfloat16)]
        + [jax.ShapeDtypeStruct((count * CAP, width), jnp.bfloat16)] * (NY - 1),
        in_specs=in_smem() + in_vmem(count),
        out_specs=in_vmem(NY),
        scratch_shapes=[pltpu.VMEM((count, NY * CAP, rows), jnp.bfloat16)],
        compiler_params=params(),
        cost_estimate=pl.CostEstimate(
            flops=2 * 96 * 128 * 4096 * count, bytes_accessed=2 * count << 20, transcendentals=0
        ),
    )(here, *slices)


def expert_kernel(steps, chunk, table_ref, *refs):
    (*ins, gate_ref, up_ref, down_ref, before_ref, out_ref, toks, grads, total) = refs
    rows, width = toks.shape
    step = pl.program_id(0)

    @pl.when(step == 0)
    def _():
        at = 0
        for part in ins:
            toks[at : at + part.shape[0], :] = part[:, :width]
            grads[at : at + part.shape[0], :] = part[:, width:]
            at += part.shape[0]

    @pl.loop(0, rows // chunk)
    def _(i):
        own = pl.ds(pl.multiple_of(i * chunk, chunk), chunk)
        x = toks[own, :]
        gate_in = jnp.dot(x, gate_ref[...], preferred_element_type=jnp.float32)
        up_in = jnp.dot(x, up_ref[...], preferred_element_type=jnp.float32)
        hidden = (gate_in / (1.0 + jnp.exp(-gate_in)) * up_in).astype(jnp.bfloat16)
        term = jnp.dot(hidden, down_ref[...], preferred_element_type=jnp.float32)

        @pl.when(step == 0)
        def _():
            total[own, :] = term

        @pl.when(step > 0)
        def _():
            total[own, :] += term

    @pl.when(step == steps - 1)
    def _():
        out_ref[...] = before_ref[...]
        lane = lax.broadcasted_iota(jnp.int32, (CAP, 128), 1)
        row = lax.broadcasted_iota(jnp.int32, (CAP, 128), 0)

        @pl.loop(0, rows // (2 * CAP))
        def _(pair):
            first = pl.multiple_of(pair * (2 * CAP), 2 * CAP)
            made = total[pl.ds(first, 2 * CAP), :].astype(jnp.bfloat16).astype(jnp.float32)
            grad = grads[pl.ds(first, 2 * CAP), :].astype(jnp.float32)
            dots = jnp.sum(made * grad, axis=1, keepdims=True)
            for half in range(2):
                home = table_ref[0, 2 * pair + half]
                source = table_ref[1, 2 * pair + half]
                mine = dots[half * CAP : (half + 1) * CAP]
                at_lane = row + (source % PACK) * STRIDE
                line = jnp.sum(jnp.where(at_lane == lane, mine, 0.0), axis=0, keepdims=True)
                out_ref[home, pl.ds(source // PACK, 1), :] += line


def expert(table, parts, gate_w, up_w, down_w, before, final):
    width, inner = gate_w.shape
    tile = 256
    steps = inner // tile
    rows = sum(part.shape[0] for part in parts)
    chunk = rows if final else 192
    return pl.pallas_call(
        functools.partial(expert_kernel, steps, chunk),
        grid=(steps,),
        out_shape=jax.ShapeDtypeStruct(before.shape, jnp.float32),
        in_specs=in_smem()
        + [pl.BlockSpec(part.shape, lambda f: (0, 0)) for part in parts]
        + [
            pl.BlockSpec((width, tile), lambda f: (0, f)),
            pl.BlockSpec((width, tile), lambda f: (0, f)),
            pl.BlockSpec((tile, width), lambda f: (f, 0)),
            pl.BlockSpec(before.shape, lambda f: (0, 0, 0)),
        ],
        out_specs=pl.BlockSpec(before.shape, lambda f: (0, 0, 0)),
        scratch_shapes=[
            pltpu.VMEM((rows, width), jnp.bfloat16),
            pltpu.VMEM((rows, width), jnp.bfloat16),
            pltpu.VMEM((rows, width), jnp.float32),
        ],
        compiler_params=params(),
        cost_estimate=pl.CostEstimate(
            flops=6 * rows * width * inner, bytes_accessed=12 << 20, transcendentals=rows * inner
        ),
    )(table, *parts, gate_w, up_w, down_w, before)


def side_kernel(keys, here_ref, *refs):
    slices, router_ref, gates_ref, place_ref, feats_ref = refs[:NZ], *refs[NZ:]
    z, c = here_ref[1], here_ref[2]
    rows = slices[0].shape[0]
    width, experts = router_ref.shape
    router = router_ref[...]
    for j in range(NZ):
        source = stop(z, c, *keys[j])
        place = slices[j][:, 2 * width :].astype(jnp.float32)[:, :experts]
        logits = jnp.dot(slices[j][:, :width], router, preferred_element_type=jnp.float32)
        hit = place >= 0.0
        weights = jnp.where(hit, jnp.exp(jnp.where(hit, logits, 0.0)), 0.0)
        gates_ref[source] = weights / jnp.sum(weights, axis=1, keepdims=True)
        place_ref[source] = place
        at = pl.multiple_of(source * rows, rows)
        for y in range(NY):
            col = pl.multiple_of(y * (width // NY) + (z // 2) * 128, 128)
            feats_ref[pl.ds(at, rows), y * 128 : (y + 1) * 128] = slices[j][:, pl.ds(col, 128)]


def side(here, keys, slices, router_weight):
    rows, experts = slices[0].shape[0], router_weight.shape[1]
    return pl.pallas_call(
        functools.partial(side_kernel, keys),
        out_shape=[
            jax.ShapeDtypeStruct((NZ, rows, experts), jnp.float32),
            jax.ShapeDtypeStruct((NZ, rows, experts), jnp.float32),
            jax.ShapeDtypeStruct((NZ * rows, NY * 128), jnp.bfloat16),
        ],
        in_specs=in_smem() + in_vmem(NZ + 1),
        out_specs=in_vmem(3),
        compiler_params=params(),
        cost_estimate=pl.CostEstimate(
            flops=2 * NZ * rows * 2048 * 256, bytes_accessed=6 << 20, transcendentals=NZ * rows * 64
        ),
    )(here, *slices, router_weight)


def finish_kernel(
    here_ref, back_ref, gates_ref, place_ref, feats_ref,
    own_ref, part_ref, table_ref, wide_ref, dense_ref, sum_ref,
):
    z = here_ref[1]
    rows, experts = gates_ref.shape[1:]
    for a in range(NZ // PACK):
        table_ref[a * 128 : (a + 1) * 128, :] = back_ref[:, a, :].T

    @pl.loop(0, NZ)
    def _(source):
        place = place_ref[source]
        lines = table_ref[pl.ds(pl.multiple_of(source * STRIDE, STRIDE), STRIDE), :]
        wide = jnp.zeros((rows, experts), jnp.float32)
        for s in range(CAP):
            wide = jnp.where(place == float(s), lines[s : s + 1, :], wide)
        wide_ref[source] = wide
        gates = gates_ref[source]
        mean = jnp.sum(gates * wide, axis=1, keepdims=True)
        at = pl.multiple_of(source * rows, rows)
        dense_ref[pl.ds(at, rows), :] = (gates * (wide - mean)).astype(jnp.bfloat16)

    part = lax.dot_general(
        dense_ref[...],
        feats_ref[...],
        (((0,), (0,)), ((), ())),
        preferred_element_type=jnp.float32,
    )
    sum_ref[...] = part.T
    half = 16
    for y in range(NY):
        for c in range(NC):
            at = pl.multiple_of(y * 128 + (z % 2) * 64 + c * 32, 32)
            for copy in range(part_ref.shape[0]):
                part_ref[copy, y * NC + c, :, :experts] = sum_ref[pl.ds(at, half), :]
                part_ref[copy, y * NC + c, :, experts:] = sum_ref[pl.ds(at + half, half), :]
    own_ref[...] = wide_ref[z]


def gate_kernel(own_ref, idx_ref, grad_ref):
    rows, experts = own_ref.shape
    number = lax.broadcasted_iota(jnp.int32, (experts, rows), 0)
    own = own_ref[...].T
    for k in range(grad_ref.shape[0]):
        here_k = idx_ref[k : k + 1, :] == number
        grad_ref[k : k + 1, :] = jnp.sum(jnp.where(here_k, own, 0.0), axis=0, keepdims=True)


def finish(here, back, gates, place, feats, copies):
    rows, experts = gates.shape[1:]
    return pl.pallas_call(
        finish_kernel,
        out_shape=[
            jax.ShapeDtypeStruct((rows, experts), jnp.float32),
            jax.ShapeDtypeStruct((copies, NY * NC, 16, 2 * experts), jnp.float32),
        ],
        in_specs=in_smem() + in_vmem(4),
        out_specs=in_vmem(2),
        scratch_shapes=[
            pltpu.VMEM((NZ * STRIDE, experts), jnp.float32),
            pltpu.VMEM((NZ, rows, experts), jnp.float32),
            pltpu.VMEM((NZ * rows, experts), jnp.bfloat16),
            pltpu.VMEM((NY * 128, experts), jnp.float32),
        ],
        compiler_params=params(),
        cost_estimate=pl.CostEstimate(flops=1 << 28, bytes_accessed=3 << 20, transcendentals=0),
    )(here, back, gates, place, feats)


def sum_kernel(parts_ref, out_ref):
    total = parts_ref[0]
    for i in range(1, parts_ref.shape[0]):
        total = total + parts_ref[i]
    half, lanes = total.shape
    out_ref[:half, :] = total[:, : lanes // 2]
    out_ref[half:, :] = total[:, lanes // 2 :]


def shifted(array, axis, by):
    size = lax.axis_size(axis)
    return lax.ppermute(array, axis, [(i, (i + by) % size) for i in range(size)])


def stop(z, core, hops, way):
    return (z + NZ + hops * (1 - 2 * core) * (2 * way - 1)) % NZ


def along_ring(array, way):
    up = (1 - 2 * way, 2 * way - 1)
    pairs = [
        (z * NC + c, (z + up[c]) % NZ * NC + c) for z in range(NZ) for c in range(NC)
    ]
    return lax.ppermute(array, ("z", "c"), pairs)


def on_device(tokens, grad_out, router_weight, expert_index, w_gate, w_up, w_down):
    tok_rows, width = tokens.shape
    experts = router_weight.shape[1]
    y, z, c = (lax.axis_index(a) for a in ("y", "z", "c"))
    here = jnp.stack([y, z, c]).astype(jnp.int32)
    packed = pl.pallas_call(
        pack_kernel,
        out_shape=jax.ShapeDtypeStruct((tok_rows, 2 * width + 128), jnp.bfloat16),
        compiler_params=params(),
    )(in_hbm(tokens), in_hbm(grad_out), expert_index.T)

    last = NZ // 2
    ring = {(0, way): packed for way in range(2)}
    for step in range(1, last + 1):
        for way in range(2 if step < last else 1):
            ring[step, way] = along_ring(ring[step - 1, way], way)
    groups = [[(0, 0)], [(1, 0)], [(1, 1)]]
    groups += [[(step, 0), (step, 1)] for step in range(2, last)] + [[(last, 0)]]
    arrived = []
    for group in groups:
        slices = [ring[key] for key in group]
        slices = slices + [shifted(a, "c", 1) for a in slices]
        rows = pick(here, slices)
        arrived.append([rows[0]] + [shifted(rows[dy], "y", dy) for dy in range(1, NY)])

    products = jnp.zeros((NY * NC, NZ // PACK, 128), jnp.float32)
    for i, members in enumerate(((0, 1, 2), (3,), (4,), (5,))):
        parts, table = [], []
        for g in members:
            for dy in range(NY):
                parts.append(arrived[g][dy])
                table += [(dy, core, *key) for core in range(NC) for key in groups[g]]
        dy, core, hops, way = np.array(table, np.int32).T
        core = (c + core) % NC
        homes = jnp.stack([(y + NY - dy) % NY * NC + core, stop(z, core, hops, way)])
        final = i == 3
        weights = [w if final else in_hbm(w) for w in (w_gate[0], w_up[0], w_down[0])]
        products = expert(homes, parts, *weights, products, final)
    gates, place, feats = side(here, list(ring)[1:], list(ring.values())[1:], router_weight)

    back = products.reshape(NY, 1, NC, NZ // PACK, 128)
    back = jnp.broadcast_to(back, (NY, NZ, NC, NZ // PACK, 128)).reshape(experts, NZ // PACK, 128)
    back = lax.all_to_all(back, ("y", "z", "c"), 0, 0, tiled=True)
    copies = lax.axis_size("dp")
    wide, part = finish(here, back, gates, place, feats, copies)
    gate_grad = pl.pallas_call(
        gate_kernel,
        out_shape=jax.ShapeDtypeStruct(expert_index.T.shape, jnp.float32),
        cost_estimate=pl.CostEstimate(flops=1 << 20, bytes_accessed=1 << 16, transcendentals=0),
    )(wide, expert_index.T).T
    parts = lax.all_to_all(
        part.reshape(copies * NY * NC, 16, 2 * experts), ("dp", "y", "c"), 0, 0, tiled=True
    )
    router_grad = pl.pallas_call(
        sum_kernel, out_shape=jax.ShapeDtypeStruct((32, experts), jnp.float32)
    )(parts)
    return (gate_grad, router_grad)


def solution(mesh):
    devices = mesh.devices.reshape(mesh.devices.shape[0], NY, NZ, NC)
    fine = Mesh(devices, ("dp", "y", "z", "c"))
    rows = P(("dp", "y", "z", "c"), None)
    own = P(("y", "z", "c"), None, None)

    return jax.shard_map(
        on_device,
        mesh=fine,
        in_specs=(rows, rows, P(), rows, own, own, own),
        out_specs=(rows, P(("y", "z", "c"), None)),
        check_vma=False,
    )
```

```python
import functools

import jax
import jax.numpy as jnp
import numpy as np
from jax import lax
from jax.experimental import pallas as pl
from jax.experimental.pallas import tpu as pltpu
from jax.sharding import Mesh, PartitionSpec as P


NY, NZ, NC = 4, 8, 2
CAP = 24
PACK, STRIDE = 4, 32
VMEM = 32 * 1024 * 1024


def params():
    return pltpu.CompilerParams(vmem_limit_bytes=VMEM)


def in_vmem(count):
    return [pl.BlockSpec(memory_space=pltpu.VMEM)] * count


def in_hbm(array):
    return pltpu.with_memory_space_constraint(array, pltpu.HBM)


def in_smem():
    return [pl.BlockSpec(memory_space=pltpu.SMEM)]


def pack_kernel(tok_ref, grad_ref, idx_ref, out_ref):
    rows, width = tok_ref.shape
    out_ref[:, :width] = tok_ref[...]
    out_ref[:, width : 2 * width] = grad_ref[...]
    label = lax.broadcasted_iota(jnp.int32, (128, rows), 0)
    hit = jnp.zeros((128, rows), jnp.float32)
    for k in range(idx_ref.shape[0]):
        hit = hit + (idx_ref[k : k + 1, :] == label).astype(jnp.float32)
    hit = hit.T
    earlier = lax.broadcasted_iota(jnp.int32, (rows, rows), 0) > lax.broadcasted_iota(
        jnp.int32, (rows, rows), 1
    )
    before = jnp.dot(
        earlier.astype(jnp.bfloat16),
        hit.astype(jnp.bfloat16),
        preferred_element_type=jnp.float32,
    )
    out_ref[:, 2 * width :] = jnp.where(hit > 0.0, before, -1.0).astype(jnp.bfloat16)


def pick_kernel(count, here_ref, *refs):
    slices, outs, chosen_ref = refs[:count], refs[count:-1], refs[-1]
    y, z, c = here_ref[0], here_ref[1], here_ref[2]
    width = outs[0].shape[1]
    slots = NY * CAP
    column = lax.broadcasted_iota(jnp.int32, (128, slots), 1)
    row = lax.broadcasted_iota(jnp.int32, (128, slots), 0)
    expert = jnp.zeros((128, slots), jnp.int32)
    slot = column
    for dy in range(NY):
        number = ((y + dy) % NY) * (NZ * NC) + z * NC + c
        expert = jnp.where(column >= dy * CAP, number, expert)
        slot = jnp.where(column >= dy * CAP, column - dy * CAP, slot)
    choose = (row == expert).astype(jnp.bfloat16)
    slot = slot.astype(jnp.float32)
    for i in range(count):
        place = slices[i][:, width:]
        spread = jnp.dot(place, choose, preferred_element_type=jnp.float32)
        chosen_ref[i] = (spread == slot).astype(jnp.float32).T.astype(jnp.bfloat16)

    tile = 1024

    @pl.loop(0, width // tile)
    def _(step):
        cols = pl.ds(pl.multiple_of(step * tile, tile), tile)
        for i in range(0, count, 2):
            taken = [
                jnp.dot(chosen_ref[j], slices[j][:, cols], preferred_element_type=jnp.float32)
                for j in (i, i + 1)
            ]
            for dy in range(NY):
                both = [t[dy * CAP : (dy + 1) * CAP] for t in taken]
                outs[dy][i * CAP : (i + 2) * CAP, cols] = jnp.concatenate(both, axis=0).astype(
                    jnp.bfloat16
                )


def pick(here, slices):
    count = len(slices)
    rows, width = slices[0].shape[0], slices[0].shape[1] - 128
    return pl.pallas_call(
        functools.partial(pick_kernel, count),
        out_shape=[pltpu.HBM((count * CAP, width), jnp.bfloat16)]
        + [jax.ShapeDtypeStruct((count * CAP, width), jnp.bfloat16)] * (NY - 1),
        in_specs=in_smem() + in_vmem(count),
        out_specs=in_vmem(NY),
        scratch_shapes=[pltpu.VMEM((count, NY * CAP, rows), jnp.bfloat16)],
        compiler_params=params(),
        cost_estimate=pl.CostEstimate(
            flops=2 * 96 * 128 * 4096 * count, bytes_accessed=2 * count << 20, transcendentals=0
        ),
    )(here, *slices)


def expert_kernel(steps, chunk, table_ref, *refs):
    (*ins, gate_ref, up_ref, down_ref, before_ref, out_ref, toks, grads, total) = refs
    rows, width = toks.shape
    step = pl.program_id(0)

    @pl.when(step == 0)
    def _():
        at = 0
        for part in ins:
            toks[at : at + part.shape[0], :] = part[:, :width]
            grads[at : at + part.shape[0], :] = part[:, width:]
            at += part.shape[0]

    @pl.loop(0, rows // chunk)
    def _(i):
        own = pl.ds(pl.multiple_of(i * chunk, chunk), chunk)
        x = toks[own, :]
        gate_in = jnp.dot(x, gate_ref[...], preferred_element_type=jnp.float32)
        up_in = jnp.dot(x, up_ref[...], preferred_element_type=jnp.float32)
        hidden = (gate_in / (1.0 + jnp.exp(-gate_in)) * up_in).astype(jnp.bfloat16)
        term = jnp.dot(hidden, down_ref[...], preferred_element_type=jnp.float32)

        @pl.when(step == 0)
        def _():
            total[own, :] = term

        @pl.when(step > 0)
        def _():
            total[own, :] += term

    @pl.when(step == steps - 1)
    def _():
        out_ref[...] = before_ref[...]
        lane = lax.broadcasted_iota(jnp.int32, (CAP, 128), 1)
        row = lax.broadcasted_iota(jnp.int32, (CAP, 128), 0)

        @pl.loop(0, rows // (2 * CAP))
        def _(pair):
            first = pl.multiple_of(pair * (2 * CAP), 2 * CAP)
            made = total[pl.ds(first, 2 * CAP), :].astype(jnp.bfloat16).astype(jnp.float32)
            grad = grads[pl.ds(first, 2 * CAP), :].astype(jnp.float32)
            dots = jnp.sum(made * grad, axis=1, keepdims=True)
            for half in range(2):
                home = table_ref[0, 2 * pair + half]
                source = table_ref[1, 2 * pair + half]
                mine = dots[half * CAP : (half + 1) * CAP]
                at_lane = row + (source % PACK) * STRIDE
                line = jnp.sum(jnp.where(at_lane == lane, mine, 0.0), axis=0, keepdims=True)
                out_ref[home, pl.ds(source // PACK, 1), :] += line


def expert(table, parts, gate_w, up_w, down_w, before, final):
    width, inner = gate_w.shape
    tile = 256
    steps = inner // tile
    rows = sum(part.shape[0] for part in parts)
    chunk = rows if final else 192
    return pl.pallas_call(
        functools.partial(expert_kernel, steps, chunk),
        grid=(steps,),
        out_shape=jax.ShapeDtypeStruct(before.shape, jnp.float32),
        in_specs=in_smem()
        + [pl.BlockSpec(part.shape, lambda f: (0, 0)) for part in parts]
        + [
            pl.BlockSpec((width, tile), lambda f: (0, f)),
            pl.BlockSpec((width, tile), lambda f: (0, f)),
            pl.BlockSpec((tile, width), lambda f: (f, 0)),
            pl.BlockSpec(before.shape, lambda f: (0, 0, 0)),
        ],
        out_specs=pl.BlockSpec(before.shape, lambda f: (0, 0, 0)),
        scratch_shapes=[
            pltpu.VMEM((rows, width), jnp.bfloat16),
            pltpu.VMEM((rows, width), jnp.bfloat16),
            pltpu.VMEM((rows, width), jnp.float32),
        ],
        compiler_params=params(),
        cost_estimate=pl.CostEstimate(
            flops=6 * rows * width * inner, bytes_accessed=12 << 20, transcendentals=rows * inner
        ),
    )(table, *parts, gate_w, up_w, down_w, before)


def side_kernel(keys, here_ref, *refs):
    slices, router_ref, gates_ref, place_ref, feats_ref = refs[:NZ], *refs[NZ:]
    z, c = here_ref[1], here_ref[2]
    rows = slices[0].shape[0]
    width, experts = router_ref.shape
    router = router_ref[...]
    for j in range(NZ):
        source = stop(z, c, *keys[j])
        place = slices[j][:, 2 * width :].astype(jnp.float32)[:, :experts]
        logits = jnp.dot(slices[j][:, :width], router, preferred_element_type=jnp.float32)
        hit = place >= 0.0
        weights = jnp.where(hit, jnp.exp(jnp.where(hit, logits, 0.0)), 0.0)
        gates_ref[source] = weights / jnp.sum(weights, axis=1, keepdims=True)
        place_ref[source] = place
        at = pl.multiple_of(source * rows, rows)
        for y in range(NY):
            col = pl.multiple_of(y * (width // NY) + (z // 2) * 128, 128)
            feats_ref[pl.ds(at, rows), y * 128 : (y + 1) * 128] = slices[j][:, pl.ds(col, 128)]


def side(here, keys, slices, router_weight):
    rows, experts = slices[0].shape[0], router_weight.shape[1]
    return pl.pallas_call(
        functools.partial(side_kernel, keys),
        out_shape=[
            jax.ShapeDtypeStruct((NZ, rows, experts), jnp.float32),
            jax.ShapeDtypeStruct((NZ, rows, experts), jnp.float32),
            jax.ShapeDtypeStruct((NZ * rows, NY * 128), jnp.bfloat16),
        ],
        in_specs=in_smem() + in_vmem(NZ + 1),
        out_specs=in_vmem(3),
        compiler_params=params(),
        cost_estimate=pl.CostEstimate(
            flops=2 * NZ * rows * 2048 * 256, bytes_accessed=6 << 20, transcendentals=NZ * rows * 64
        ),
    )(here, *slices, router_weight)


def finish_kernel(
    here_ref, back_ref, gates_ref, place_ref, feats_ref,
    own_ref, part_ref, table_ref, wide_ref, dense_ref, sum_ref,
):
    z = here_ref[1]
    rows, experts = gates_ref.shape[1:]
    for a in range(NZ // PACK):
        table_ref[a * 128 : (a + 1) * 128, :] = back_ref[:, a, :].T

    @pl.loop(0, NZ)
    def _(source):
        place = place_ref[source]
        lines = table_ref[pl.ds(pl.multiple_of(source * STRIDE, STRIDE), STRIDE), :]
        wide = jnp.zeros((rows, experts), jnp.float32)
        for s in range(CAP):
            wide = jnp.where(place == float(s), lines[s : s + 1, :], wide)
        wide_ref[source] = wide
        gates = gates_ref[source]
        mean = jnp.sum(gates * wide, axis=1, keepdims=True)
        at = pl.multiple_of(source * rows, rows)
        dense_ref[pl.ds(at, rows), :] = (gates * (wide - mean)).astype(jnp.bfloat16)

    part = lax.dot_general(
        dense_ref[...],
        feats_ref[...],
        (((0,), (0,)), ((), ())),
        preferred_element_type=jnp.float32,
    )
    sum_ref[...] = part.T
    half = 16
    for y in range(NY):
        for c in range(NC):
            at = pl.multiple_of(y * 128 + (z % 2) * 64 + c * 32, 32)
            for copy in range(part_ref.shape[0]):
                part_ref[copy, y * NC + c, :, :experts] = sum_ref[pl.ds(at, half), :]
                part_ref[copy, y * NC + c, :, experts:] = sum_ref[pl.ds(at + half, half), :]
    own_ref[...] = wide_ref[z]


def gate_kernel(own_ref, idx_ref, grad_ref):
    rows, experts = own_ref.shape
    number = lax.broadcasted_iota(jnp.int32, (experts, rows), 0)
    own = own_ref[...].T
    for k in range(grad_ref.shape[0]):
        here_k = idx_ref[k : k + 1, :] == number
        grad_ref[k : k + 1, :] = jnp.sum(jnp.where(here_k, own, 0.0), axis=0, keepdims=True)


def finish(here, back, gates, place, feats, copies):
    rows, experts = gates.shape[1:]
    return pl.pallas_call(
        finish_kernel,
        out_shape=[
            pltpu.HBM((rows, experts), jnp.float32),
            jax.ShapeDtypeStruct((copies, NY * NC, 16, 2 * experts), jnp.float32),
        ],
        in_specs=in_smem() + in_vmem(4),
        out_specs=in_vmem(2),
        scratch_shapes=[
            pltpu.VMEM((NZ * STRIDE, experts), jnp.float32),
            pltpu.VMEM((NZ, rows, experts), jnp.float32),
            pltpu.VMEM((NZ * rows, experts), jnp.bfloat16),
            pltpu.VMEM((NY * 128, experts), jnp.float32),
        ],
        compiler_params=params(),
        cost_estimate=pl.CostEstimate(flops=1 << 28, bytes_accessed=3 << 20, transcendentals=0),
    )(here, back, gates, place, feats)


def sum_kernel(parts_ref, out_ref):
    total = parts_ref[0]
    for i in range(1, parts_ref.shape[0]):
        total = total + parts_ref[i]
    half, lanes = total.shape
    out_ref[:half, :] = total[:, : lanes // 2]
    out_ref[half:, :] = total[:, lanes // 2 :]


def shifted(array, axis, by):
    size = lax.axis_size(axis)
    return lax.ppermute(array, axis, [(i, (i + by) % size) for i in range(size)])


def stop(z, core, hops, way):
    return (z + NZ + hops * (1 - 2 * core) * (2 * way - 1)) % NZ


def along_ring(array, way):
    up = (1 - 2 * way, 2 * way - 1)
    pairs = [
        (z * NC + c, (z + up[c]) % NZ * NC + c) for z in range(NZ) for c in range(NC)
    ]
    return lax.ppermute(array, ("z", "c"), pairs)


def on_device(tokens, grad_out, router_weight, expert_index, w_gate, w_up, w_down):
    tok_rows, width = tokens.shape
    experts = router_weight.shape[1]
    y, z, c = (lax.axis_index(a) for a in ("y", "z", "c"))
    here = jnp.stack([y, z, c]).astype(jnp.int32)
    packed = pl.pallas_call(
        pack_kernel,
        out_shape=jax.ShapeDtypeStruct((tok_rows, 2 * width + 128), jnp.bfloat16),
        compiler_params=params(),
    )(in_hbm(tokens), in_hbm(grad_out), expert_index.T)

    last = NZ // 2
    ring = {(0, way): packed for way in range(2)}
    for step in range(1, last + 1):
        for way in range(2 if step < last else 1):
            ring[step, way] = along_ring(ring[step - 1, way], way)
    groups = [[(0, 0)], [(1, 0)], [(1, 1)]]
    groups += [[(step, 0), (step, 1)] for step in range(2, last)] + [[(last, 0)]]
    arrived = []
    for group in groups:
        slices = [ring[key] for key in group]
        slices = slices + [shifted(a, "c", 1) for a in slices]
        rows = pick(here, slices)
        near = [shifted(rows[dy], "y", dy) for dy in (1, 3)]
        far = shifted(rows[2], "y", 2)
        arrived.append([rows[0], near[0], far, near[1]])

    products = jnp.zeros((NY * NC, NZ // PACK, 128), jnp.float32)
    for i, members in enumerate(((0, 1, 2), (3,), (4,), (5,))):
        parts, table = [], []
        for g in members:
            for dy in range(NY):
                parts.append(arrived[g][dy])
                table += [(dy, core, *key) for core in range(NC) for key in groups[g]]
        dy, core, hops, way = np.array(table, np.int32).T
        core = (c + core) % NC
        homes = jnp.stack([(y + NY - dy) % NY * NC + core, stop(z, core, hops, way)])
        final = i == 3
        weights = [w if final else in_hbm(w) for w in (w_gate[0], w_up[0], w_down[0])]
        products = expert(homes, parts, *weights, products, final)
    gates, place, feats = side(here, list(ring)[1:], list(ring.values())[1:], router_weight)

    back = products.reshape(NY, 1, NC, NZ // PACK, 128)
    back = jnp.broadcast_to(back, (NY, NZ, NC, NZ // PACK, 128)).reshape(experts, NZ // PACK, 128)
    back = lax.all_to_all(back, ("y", "z", "c"), 0, 0, tiled=True)
    copies = lax.axis_size("dp")
    wide, part = finish(here, back, gates, place, feats, copies)
    gate_grad = pl.pallas_call(
        gate_kernel,
        out_shape=jax.ShapeDtypeStruct(expert_index.T.shape, jnp.float32),
        cost_estimate=pl.CostEstimate(flops=1 << 20, bytes_accessed=1 << 16, transcendentals=0),
    )(wide, expert_index.T).T
    parts = lax.all_to_all(
        part.reshape(copies * NY * NC, 16, 2 * experts), ("dp", "y", "c"), 0, 0, tiled=True
    )
    router_grad = pl.pallas_call(
        sum_kernel, out_shape=jax.ShapeDtypeStruct((32, experts), jnp.float32)
    )(in_hbm(parts))
    return (gate_grad, router_grad)


def solution(mesh):
    devices = mesh.devices.reshape(mesh.devices.shape[0], NY, NZ, NC)
    fine = Mesh(devices, ("dp", "y", "z", "c"))
    rows = P(("dp", "y", "z", "c"), None)
    own = P(("y", "z", "c"), None, None)

    return jax.shard_map(
        on_device,
        mesh=fine,
        in_specs=(rows, rows, P(), rows, own, own, own),
        out_specs=(rows, P(("y", "z", "c"), None)),
        check_vma=False,
    )
```
